32 devices in a mesh: row: 4 (over z), col: 8 (over y, x, core).
Axes of the slice: x: 2, y: 2, z: 4, core: 2. Of those that a mesh axis runs over, the one named last changes fastest.
Arguments:
- matrix: float32 [8192, 8192], P('row', 'col'), may hold values from -2.5 to 2.5
Outputs:
- squared: float32 [8192, 8192], P('row', 'col')
- frob: float32 [], replicated
The draws below stay inside these ranges and needn't reach their ends.
All inputs are finite; a program needn't handle non-finite values.
Results may differ from the reference program's by a relative error of at most 0.0001.
Values sent between devices are 32-bit elements; how exact they have to be, the bound alone decides.
A program may use at most 64 MiB of HBM per device.

```python
import jax
import jax.numpy as jnp
from jax import lax

N = 8192
KP = 256


def steps_of(key, shape, cuts, low, largest):
    gain = 1.0
    for axis_at, parts in cuts:
        draws = jax.random.uniform(jax.random.fold_in(jax.random.fold_in(key, 6), axis_at), (parts,), jnp.float32, low / len(cuts), largest / len(cuts))
        gain = gain * jnp.repeat(jnp.exp(draws), shape[axis_at] // parts).reshape((-1,) + (1,) * (len(shape) - 1 - axis_at))
    return gain


def noise(rng, extent, scale, reach, shards=(), kind=jnp.bfloat16):
    entries = scale * jax.random.normal(rng, extent, jnp.float32)
    if shards:
        entries = entries * steps_of(rng, extent, shards, -0.22, 0.18)
    return jnp.clip(entries, -reach, reach).astype(kind)


def setup_inputs(seed: int = 0) -> dict:
    key_list = jax.random.split(jax.random.key(seed), 2)
    return {
        "matrix": noise(key_list[0], (N, N), ((4 * KP) ** -0.25), 2.5, ((0, 4), (1, 8)), jnp.float32),
    }


def reference(matrix):
    stride = N // 4
    squared = jnp.zeros((N, N), jnp.float32)
    for step in range(4):
        start = step * stride
        squared = squared + jnp.dot(matrix[:, start:start + KP], matrix[start:start + KP, :], preferred_element_type=jnp.float32, precision=lax.Precision.HIGHEST)
    frob = jnp.sqrt(jnp.sum(squared * squared)) / N
    return (squared, frob)
```

```python
import functools

import jax
import jax.numpy as jnp
from jax import lax
from jax.experimental import pallas as pl
from jax.experimental.pallas import tpu as pltpu
from jax.sharding import PartitionSpec as P

KP = 256
PANELS = 4
MESH = pl.DeviceIdType.MESH


def kernel(
    rows_n, cols_n, order, pieces, x_ref, out_ref, frob_ref, right, left, high, low, part_col, part_row,
    local_sem, z_recv, z_up, z_down, pair_send, pair_recv, hop_send, hop_recv, relay_send, relay_recv,
    col_send, col_recv, row_send, row_recv,
):
    row = lax.axis_index("row")
    col = lax.axis_index("col")
    chip = col // 2
    core = col % 2
    partner = chip * 2 + 1 - core
    row_block, col_block = out_ref.shape
    half = row_block // 2
    width = col_block // pieces

    barrier = pltpu.get_barrier_semaphore()
    for d in range(1, cols_n):
        pl.semaphore_signal(barrier, inc=1, device_id=(row, lax.rem(col + d, cols_n)), device_id_type=MESH)
    for d in range(1, rows_n):
        pl.semaphore_signal(barrier, inc=1, device_id=(lax.rem(row + d, rows_n), col), device_id_type=MESH)
    pl.semaphore_wait(barrier, rows_n + cols_n - 2)

    def columns(j):
        return pl.ds(pl.multiple_of(j * width, width), width)

    def z_copy(s, j, sems, target, own):
        view = right.at[s, :, columns(j)]
        source = x_ref.at[pl.ds(0, KP), columns(j)] if own else view
        return pltpu.make_async_remote_copy(
            src_ref=source, dst_ref=view, send_sem=sems.at[s, j], recv_sem=z_recv.at[s, j],
            device_id=(target, col), device_id_type=MESH,
        )

    above = lax.min(row + 1, rows_n - 1)
    below = lax.max(row - 1, 0)
    has_above = row < rows_n - 1
    has_below = row > 0

    def start_own(j, carry):
        @pl.when(has_above)
        def _():
            z_copy(row, j, z_up, above, True).start()

        @pl.when(has_below)
        def _():
            z_copy(row, j, z_down, below, True).start()

        return carry

    lax.fori_loop(0, pieces, start_own, 0)

    def pair_copy():
        return pltpu.make_async_remote_copy(
            src_ref=x_ref.at[:, pl.ds(0, KP)], dst_ref=left.at[chip], send_sem=pair_send, recv_sem=pair_recv,
            device_id=(row, partner), device_id_type=MESH,
        )

    def flip(q, d):
        hi, lo = q // 2, q % 2
        hi = hi if d < 2 else 1 - hi
        lo = lo if d % 2 == 0 else 1 - lo
        return hi * 2 + lo

    def hop_copy(d, h):
        rows = pl.ds(h * half, half)
        return pltpu.make_async_remote_copy(
            src_ref=x_ref.at[rows, pl.ds(0, KP)], dst_ref=left.at[chip, rows, :],
            send_sem=hop_send.at[d, h], recv_sem=hop_recv.at[chip],
            device_id=(row, flip(chip, d) * 2 + h), device_id_type=MESH,
        )

    @pl.when(core == 0)
    def _():
        for d in (1, 2, 3):
            for h in (0, 1):
                hop_copy(d, h).start()
        pair_copy().start()

    own_right = pltpu.make_async_copy(x_ref.at[pl.ds(0, KP), :], right.at[row], local_sem.at[0])
    own_left = pltpu.make_async_copy(x_ref.at[:, pl.ds(0, KP)], left.at[chip], local_sem.at[1])
    own_right.start()

    @pl.when(core == 0)
    def _():
        own_left.start()

    tile = 256
    tiles = row_block // tile

    def clear(i, carry):
        out_ref[pl.ds(pl.multiple_of(i * tile, tile), tile), :] = jnp.zeros((tile, col_block), jnp.float32)
        return carry

    lax.fori_loop(0, tiles, clear, 0)

    def split(s):
        def one(i, carry):
            rows = pl.ds(pl.multiple_of(i * tile, tile), tile)
            value = left[s, rows, :]
            head = value.astype(jnp.bfloat16)
            high[s, rows, :] = head
            low[s, rows, :] = (value - head.astype(jnp.float32)).astype(jnp.bfloat16)
            return carry

        lax.fori_loop(0, tiles, one, 0)

    def multiply(s, j):
        cols = columns(j)
        value = right[s, :, cols]
        head = value.astype(jnp.bfloat16)
        tail = (value - head.astype(jnp.float32)).astype(jnp.bfloat16)

        def one(i, carry):
            rows = pl.ds(pl.multiple_of(i * tile, tile), tile)
            a, b = high[s, rows, :], low[s, rows, :]
            dot = functools.partial(jnp.dot, preferred_element_type=jnp.float32)
            out_ref[rows, cols] += dot(a, head) + (dot(a, tail) + dot(b, head))
            return carry

        lax.fori_loop(0, tiles, one, 0)

    def receive(k, j):
        @pl.when(row >= k)
        def _():
            s = lax.max(row - k, 0)
            z_copy(s, j, z_up, above, False).wait_recv()

            @pl.when(has_above)
            def _():
                z_copy(s, j, z_up, above, False).start()

        @pl.when(row + k < rows_n)
        def _():
            s = lax.min(row + k, rows_n - 1)
            z_copy(s, j, z_down, below, False).wait_recv()

            @pl.when(has_below)
            def _():
                z_copy(s, j, z_down, below, False).start()

    def compute(k, j):
        @pl.when(row >= k)
        def _():
            multiply(lax.max(row - k, 0), j)

        @pl.when(row + k < rows_n)
        def _():
            multiply(lax.min(row + k, rows_n - 1), j)

    mine = pl.ds(pl.multiple_of(core * half, half), half)
    other = pl.ds(pl.multiple_of((1 - core) * half, half), half)

    def relay_copy(s, rows):
        return pltpu.make_async_remote_copy(
            src_ref=left.at[s, rows, :], dst_ref=left.at[s, rows, :], send_sem=relay_send.at[s],
            recv_sem=relay_recv.at[s], device_id=(row, partner), device_id_type=MESH,
        )

    def hop_arrival(s):
        view = left.at[s, mine, :]
        return pltpu.make_async_remote_copy(
            src_ref=view, dst_ref=view, send_sem=hop_send.at[0, 0], recv_sem=hop_recv.at[s],
            device_id=(row, partner), device_id_type=MESH,
        )

    def relay(distances):
        for d in distances:
            s = flip(chip, d)
            hop_arrival(s).wait_recv()
            relay_copy(s, mine).start()
        for d in distances:
            s = flip(chip, d)
            relay_copy(s, other).wait_recv()
            relay_copy(s, mine).wait_send()
            split(s)

    own_right.wait()

    @pl.when(core == 0)
    def _():
        own_left.wait()

    @pl.when(core == 1)
    def _():
        pair_copy().wait_recv()

    split(chip)

    def step(k, work):
        def one(j, carry):
            receive(k, j)
            if work:
                compute(k, j)
            return carry

        lax.fori_loop(0, pieces, one, 0)

    step(1, False)
    relay((1, 2))
    step(2, False)
    relay((3,))

    def early(j, carry):
        multiply(row, j)
        compute(1, j)
        compute(2, j)
        return carry

    lax.fori_loop(0, pieces, early, 0)

    def last(j, total):
        for k in range(3, rows_n):
            receive(k, j)
            compute(k, j)
        cols = columns(j)

        def one(i, acc):
            value = out_ref[pl.ds(pl.multiple_of(i * tile, tile), tile), cols]
            value = value * value
            return acc + jnp.sum(value.reshape(tile // 8, 8, width), axis=0)

        return lax.fori_loop(0, tiles, one, total)

    total = lax.fori_loop(0, pieces, last, jnp.zeros((8, width), jnp.float32))
    part_col[col] = sum(total[:, i * 128 : (i + 1) * 128] for i in range(width // 128))

    def drain(j, carry):
        @pl.when(has_above)
        def _():
            z_copy(row, j, z_up, above, True).wait_send()

        @pl.when(has_below)
        def _():
            z_copy(row, j, z_down, below, True).wait_send()

        for k in range(1, rows_n):
            @pl.when(jnp.logical_and(row >= k, has_above))
            def _():
                z_copy(lax.max(row - k, 0), j, z_up, above, False).wait_send()

            @pl.when(jnp.logical_and(row + k < rows_n, has_below))
            def _():
                z_copy(lax.min(row + k, rows_n - 1), j, z_down, below, False).wait_send()

        return carry

    lax.fori_loop(0, pieces, drain, 0)

    @pl.when(core == 0)
    def _():
        for d in (1, 2, 3):
            for h in (0, 1):
                hop_copy(d, h).wait_send()
        pair_copy().wait_send()

    def spread(part, place, count, send, recv, device):
        def copy(d, slot):
            return pltpu.make_async_remote_copy(
                src_ref=part.at[slot], dst_ref=part.at[slot], send_sem=send.at[d], recv_sem=recv.at[slot],
                device_id=device(lax.rem(place + d, count)), device_id_type=MESH,
            )

        for d in range(1, count):
            copy(d, place).start()
        for d in range(1, count):
            copy(d, lax.rem(place + d, count)).wait_recv()
        for d in range(1, count):
            copy(d, place).wait_send()

    spread(part_col, col, cols_n, col_send, col_recv, lambda c: (row, c))
    part_row[row] = jnp.sum(part_col[...], axis=0)
    spread(part_row, row, rows_n, row_send, row_recv, lambda r: (r, col))
    full = jnp.sum(jnp.sum(part_row[...], axis=0), keepdims=True)
    frob_ref[...] = jnp.sqrt(full) / order


def fused(rows_n, cols_n, matrix):
    row_block, col_block = matrix.shape
    order = row_block * rows_n
    pieces = max(1, col_block // 256)
    dma = pltpu.SemaphoreType.DMA
    vmem = pl.BlockSpec(memory_space=pltpu.VMEM)
    squared, frob = pl.pallas_call(
        functools.partial(kernel, rows_n, cols_n, order, pieces),
        out_shape=(
            jax.ShapeDtypeStruct((row_block, col_block), jnp.float32),
            jax.ShapeDtypeStruct((1, 1), jnp.float32),
        ),
        in_specs=[pl.BlockSpec(memory_space=pltpu.HBM)],
        out_specs=(vmem, vmem),
        scratch_shapes=[
            pltpu.VMEM((PANELS, KP, col_block), jnp.float32),
            pltpu.VMEM((PANELS, row_block, KP), jnp.float32),
            pltpu.VMEM((PANELS, row_block, KP), jnp.bfloat16),
            pltpu.VMEM((PANELS, row_block, KP), jnp.bfloat16),
            pltpu.VMEM((cols_n, 8, 128), jnp.float32),
            pltpu.VMEM((rows_n, 8, 128), jnp.float32),
            dma((2,)), dma((PANELS, pieces)), dma((PANELS, pieces)), dma((PANELS, pieces)),
            dma(()), dma(()), dma((PANELS, 2)), dma((PANELS,)), dma((PANELS,)), dma((PANELS,)),
            dma((cols_n,)), dma((cols_n,)), dma((rows_n,)), dma((rows_n,)),
        ],
        compiler_params=pltpu.CompilerParams(
            collective_id=0, has_side_effects=True, vmem_limit_bytes=60 * 1024 * 1024
        ),
    )(matrix)
    return squared, frob.reshape(())


def broadcast(value, axis, source):
    kept = jnp.where(lax.axis_index(axis) == source, value, 0).astype(value.dtype)
    return lax.psum(kept, axis)


def offsets(matrix, step):
    row_block = matrix.shape[0]
    col_block = matrix.shape[1]
    total = row_block * lax.axis_size("row")
    start = step * (total // PANELS)
    return (start // col_block, start % col_block, start // row_block, start % row_block)


def fetch_rows(matrix, step):
    col_owner, local_col, row_owner, local_row = offsets(matrix, step)
    return broadcast(matrix[local_row : local_row + KP, :], "row", row_owner)


def product(left, right):
    return jnp.dot(left, right, preferred_element_type=jnp.float32, precision=lax.Precision.HIGHEST)


def general(matrix):
    column_index = lax.axis_index("col")
    slots = []
    for step in range(PANELS):
        col_owner, local_col, row_owner, local_row = offsets(matrix, step)
        panel = matrix[:, local_col : local_col + KP]
        slots.append(jnp.where(column_index == col_owner, panel, jnp.zeros_like(panel)))
    stacked = lax.psum(jnp.concatenate(slots, axis=1), "col")
    rights = jnp.concatenate([fetch_rows(matrix, step) for step in range(PANELS)], axis=0)
    squared = product(stacked, rights)
    total = lax.psum(jnp.sum(squared * squared), ("row", "col"))
    order_size = matrix.shape[0] * lax.axis_size("row")
    frob = jnp.sqrt(total) / order_size
    return (squared, frob)


def solution(mesh):
    rows_n, cols_n = mesh.shape["row"], mesh.shape["col"]
    if rows_n == PANELS and cols_n == 2 * PANELS:
        body = functools.partial(fused, rows_n, cols_n)
    else:
        body = general
    return jax.shard_map(
        body, mesh=mesh, in_specs=(P("row", "col"),), out_specs=(P("row", "col"), P()), check_vma=False
    )
```

```python
import functools

import jax
import jax.numpy as jnp
from jax import lax
from jax.experimental import pallas as pl
from jax.experimental.pallas import tpu as pltpu
from jax.sharding import PartitionSpec as P

KP = 256
PANELS = 4
DOT = 1024
MESH = pl.DeviceIdType.MESH


def kernel(
    rows_n, cols_n, order, pieces, x_ref, out_ref, frob_ref, right, left, halves, weights, part_col, part_row,
    local_sem, z_recv, z_up, z_down, pair_send, pair_recv, hop_send, hop_recv, relay_send, relay_recv,
    col_send, col_recv, row_send, row_recv,
):
    row = lax.axis_index("row")
    col = lax.axis_index("col")
    chip = col // 2
    core = col % 2
    partner = chip * 2 + 1 - core
    row_block, col_block = out_ref.shape
    half = row_block // 2
    width = col_block // pieces

    barrier = pltpu.get_barrier_semaphore()
    for d in range(1, cols_n):
        pl.semaphore_signal(barrier, inc=1, device_id=(row, lax.rem(col + d, cols_n)), device_id_type=MESH)
    for d in range(1, rows_n):
        pl.semaphore_signal(barrier, inc=1, device_id=(lax.rem(row + d, rows_n), col), device_id_type=MESH)
    pl.semaphore_wait(barrier, rows_n + cols_n - 2)

    def columns(j):
        return pl.ds(pl.multiple_of(j * width, width), width)

    def z_copy(s, j, sems, target, own):
        view = right.at[s, :, columns(j)]
        source = x_ref.at[pl.ds(0, KP), columns(j)] if own else view
        return pltpu.make_async_remote_copy(
            src_ref=source, dst_ref=view, send_sem=sems.at[s, j], recv_sem=z_recv.at[s, j],
            device_id=(target, col), device_id_type=MESH,
        )

    above = lax.min(row + 1, rows_n - 1)
    below = lax.max(row - 1, 0)
    has_above = row < rows_n - 1
    has_below = row > 0

    def start_own(j, carry):
        @pl.when(has_above)
        def _():
            z_copy(row, j, z_up, above, True).start()

        @pl.when(has_below)
        def _():
            z_copy(row, j, z_down, below, True).start()

        return carry

    lax.fori_loop(0, pieces, start_own, 0)

    def pair_copy():
        return pltpu.make_async_remote_copy(
            src_ref=x_ref.at[:, pl.ds(0, KP)], dst_ref=left.at[chip], send_sem=pair_send, recv_sem=pair_recv,
            device_id=(row, partner), device_id_type=MESH,
        )

    def flip(q, d):
        hi, lo = q // 2, q % 2
        hi = hi if d < 2 else 1 - hi
        lo = lo if d % 2 == 0 else 1 - lo
        return hi * 2 + lo

    def hop_copy(d, h):
        rows = pl.ds(h * half, half)
        return pltpu.make_async_remote_copy(
            src_ref=x_ref.at[rows, pl.ds(0, KP)], dst_ref=left.at[chip, rows, :],
            send_sem=hop_send.at[d, h], recv_sem=hop_recv.at[chip],
            device_id=(row, flip(chip, d) * 2 + h), device_id_type=MESH,
        )

    @pl.when(core == 0)
    def _():
        for d in (1, 2, 3):
            for h in (0, 1):
                hop_copy(d, h).start()
        pair_copy().start()

    own_right = pltpu.make_async_copy(x_ref.at[pl.ds(0, KP), :], right.at[row], local_sem.at[0])
    own_left = pltpu.make_async_copy(x_ref.at[:, pl.ds(0, KP)], left.at[chip], local_sem.at[1])
    own_right.start()

    @pl.when(core == 0)
    def _():
        own_left.start()

    tile = 256
    tiles = row_block // tile

    def split(s):
        def one(i, carry):
            rows = pl.ds(pl.multiple_of(i * tile, tile), tile)
            value = left[s, rows, :]
            head = value.astype(jnp.bfloat16)
            halves[s, rows, pl.ds(0, KP)] = head
            halves[s, rows, pl.ds(KP, KP)] = (value - head.astype(jnp.float32)).astype(jnp.bfloat16)
            return carry

        lax.fori_loop(0, tiles, one, 0)

    def multiply(first, count, j, add):
        cols = columns(j)
        for i in range(count):
            value = right[first + i, :, cols]
            head = value.astype(jnp.bfloat16)
            weights[pl.ds(3 * KP * i, KP), :] = head
            weights[pl.ds(3 * KP * i + KP, KP), :] = head
            weights[pl.ds(3 * KP * i + 2 * KP, KP), :] = (value - head.astype(jnp.float32)).astype(jnp.bfloat16)

        def one(i, carry):
            rows = pl.ds(pl.multiple_of(i * DOT, DOT), DOT)
            pieces_of = []
            for p in range(count):
                pieces_of += [halves[first + p, rows, :], halves[first + p, rows, pl.ds(0, KP)]]
            value = jnp.dot(
                jnp.concatenate(pieces_of, axis=1), weights[pl.ds(0, 3 * KP * count), :],
                preferred_element_type=jnp.float32,
            )
            out_ref[rows, cols] = value + out_ref[rows, cols] if add else value
            return carry

        lax.fori_loop(0, row_block // DOT, one, 0)

    def receive(k, j):
        @pl.when(row >= k)
        def _():
            s = lax.max(row - k, 0)
            z_copy(s, j, z_up, above, False).wait_recv()

            @pl.when(has_above)
            def _():
                z_copy(s, j, z_up, above, False).start()

        @pl.when(row + k < rows_n)
        def _():
            s = lax.min(row + k, rows_n - 1)
            z_copy(s, j, z_down, below, False).wait_recv()

            @pl.when(has_below)
            def _():
                z_copy(s, j, z_down, below, False).start()

    mine = pl.ds(pl.multiple_of(core * half, half), half)
    other = pl.ds(pl.multiple_of((1 - core) * half, half), half)

    def relay_copy(s, rows):
        return pltpu.make_async_remote_copy(
            src_ref=left.at[s, rows, :], dst_ref=left.at[s, rows, :], send_sem=relay_send.at[s],
            recv_sem=relay_recv.at[s], device_id=(row, partner), device_id_type=MESH,
        )

    def hop_arrival(s):
        view = left.at[s, mine, :]
        return pltpu.make_async_remote_copy(
            src_ref=view, dst_ref=view, send_sem=hop_send.at[0, 0], recv_sem=hop_recv.at[s],
            device_id=(row, partner), device_id_type=MESH,
        )

    def relay(distances):
        for d in distances:
            s = flip(chip, d)
            hop_arrival(s).wait_recv()
            relay_copy(s, mine).start()
        for d in distances:
            s = flip(chip, d)
            relay_copy(s, other).wait_recv()
            relay_copy(s, mine).wait_send()
            split(s)

    own_right.wait()

    @pl.when(core == 0)
    def _():
        own_left.wait()

    @pl.when(core == 1)
    def _():
        pair_copy().wait_recv()

    split(chip)

    def step(k):
        def one(j, carry):
            receive(k, j)
            return carry

        lax.fori_loop(0, pieces, one, 0)

    step(1)
    relay((1, 2))
    step(2)
    relay((3,))

    low_end = row < rows_n // 2
    first = jnp.where(low_end, 0, 1)
    farthest = jnp.where(low_end, rows_n - 1, 0)

    def early(j, carry):
        multiply(first, PANELS - 1, j, False)
        return carry

    lax.fori_loop(0, pieces, early, 0)

    def last(j, total):
        receive(rows_n - 1, j)
        multiply(farthest, 1, j, True)
        cols = columns(j)

        def one(i, acc):
            value = out_ref[pl.ds(pl.multiple_of(i * tile, tile), tile), cols]
            value = value * value
            return acc + jnp.sum(value.reshape(tile // 8, 8, width), axis=0)

        return lax.fori_loop(0, tiles, one, total)

    total = lax.fori_loop(0, pieces, last, jnp.zeros((8, width), jnp.float32))
    part_col[col] = sum(total[:, i * 128 : (i + 1) * 128] for i in range(width // 128))

    def drain(j, carry):
        @pl.when(has_above)
        def _():
            z_copy(row, j, z_up, above, True).wait_send()

        @pl.when(has_below)
        def _():
            z_copy(row, j, z_down, below, True).wait_send()

        for k in range(1, rows_n):
            @pl.when(jnp.logical_and(row >= k, has_above))
            def _():
                z_copy(lax.max(row - k, 0), j, z_up, above, False).wait_send()

            @pl.when(jnp.logical_and(row + k < rows_n, has_below))
            def _():
                z_copy(lax.min(row + k, rows_n - 1), j, z_down, below, False).wait_send()

        return carry

    lax.fori_loop(0, pieces, drain, 0)

    @pl.when(core == 0)
    def _():
        for d in (1, 2, 3):
            for h in (0, 1):
                hop_copy(d, h).wait_send()
        pair_copy().wait_send()

    def spread(part, place, count, send, recv, device):
        def copy(d, slot):
            return pltpu.make_async_remote_copy(
                src_ref=part.at[slot], dst_ref=part.at[slot], send_sem=send.at[d], recv_sem=recv.at[slot],
                device_id=device(lax.rem(place + d, count)), device_id_type=MESH,
            )

        for d in range(1, count):
            copy(d, place).start()
        for d in range(1, count):
            copy(d, lax.rem(place + d, count)).wait_recv()
        for d in range(1, count):
            copy(d, place).wait_send()

    spread(part_col, col, cols_n, col_send, col_recv, lambda c: (row, c))
    part_row[row] = jnp.sum(part_col[...], axis=0)
    spread(part_row, row, rows_n, row_send, row_recv, lambda r: (r, col))
    full = jnp.sum(jnp.sum(part_row[...], axis=0), keepdims=True)
    frob_ref[...] = jnp.sqrt(full) / order


def fused(rows_n, cols_n, matrix):
    row_block, col_block = matrix.shape
    order = row_block * rows_n
    pieces = max(1, col_block // 256)
    dma = pltpu.SemaphoreType.DMA
    vmem = pl.BlockSpec(memory_space=pltpu.VMEM)
    squared, frob = pl.pallas_call(
        functools.partial(kernel, rows_n, cols_n, order, pieces),
        out_shape=(
            pltpu.VMEM((row_block, col_block), jnp.float32),
            jax.ShapeDtypeStruct((1, 1), jnp.float32),
        ),
        in_specs=[pl.BlockSpec(memory_space=pltpu.HBM)],
        out_specs=(vmem, vmem),
        scratch_shapes=[
            pltpu.VMEM((PANELS, KP, col_block), jnp.float32),
            pltpu.VMEM((PANELS, row_block, KP), jnp.float32),
            pltpu.VMEM((PANELS, row_block, 2 * KP), jnp.bfloat16),
            pltpu.VMEM((3 * KP * (PANELS - 1), col_block // pieces), jnp.bfloat16),
            pltpu.VMEM((cols_n, 8, 128), jnp.float32),
            pltpu.VMEM((rows_n, 8, 128), jnp.float32),
            dma((2,)), dma((PANELS, pieces)), dma((PANELS, pieces)), dma((PANELS, pieces)),
            dma(()), dma(()), dma((PANELS, 2)), dma((PANELS,)), dma((PANELS,)), dma((PANELS,)),
            dma((cols_n,)), dma((cols_n,)), dma((rows_n,)), dma((rows_n,)),
        ],
        compiler_params=pltpu.CompilerParams(
            collective_id=0, has_side_effects=True, vmem_limit_bytes=52 * 1024 * 1024
        ),
    )(matrix)
    return squared, frob.reshape(())


def broadcast(value, axis, source):
    kept = jnp.where(lax.axis_index(axis) == source, value, 0).astype(value.dtype)
    return lax.psum(kept, axis)


def offsets(matrix, step):
    row_block = matrix.shape[0]
    col_block = matrix.shape[1]
    total = row_block * lax.axis_size("row")
    start = step * (total // PANELS)
    return (start // col_block, start % col_block, start // row_block, start % row_block)


def fetch_rows(matrix, step):
    col_owner, local_col, row_owner, local_row = offsets(matrix, step)
    return broadcast(matrix[local_row : local_row + KP, :], "row", row_owner)


def product(left, right):
    return jnp.dot(left, right, preferred_element_type=jnp.float32, precision=lax.Precision.HIGHEST)


def general(matrix):
    column_index = lax.axis_index("col")
    slots = []
    for step in range(PANELS):
        col_owner, local_col, row_owner, local_row = offsets(matrix, step)
        panel = matrix[:, local_col : local_col + KP]
        slots.append(jnp.where(column_index == col_owner, panel, jnp.zeros_like(panel)))
    stacked = lax.psum(jnp.concatenate(slots, axis=1), "col")
    rights = jnp.concatenate([fetch_rows(matrix, step) for step in range(PANELS)], axis=0)
    squared = product(stacked, rights)
    total = lax.psum(jnp.sum(squared * squared), ("row", "col"))
    order_size = matrix.shape[0] * lax.axis_size("row")
    frob = jnp.sqrt(total) / order_size
    return (squared, frob)


def solution(mesh):
    rows_n, cols_n = mesh.shape["row"], mesh.shape["col"]
    if rows_n == PANELS and cols_n == 2 * PANELS:
        body = functools.partial(fused, rows_n, cols_n)
    else:
        body = general
    return jax.shard_map(
        body, mesh=mesh, in_specs=(P("row", "col"),), out_specs=(P("row", "col"), P()), check_vma=False
    )
```

```python
import functools

import jax
import jax.numpy as jnp
from jax import lax
from jax.experimental import pallas as pl
from jax.experimental.pallas import tpu as pltpu
from jax.sharding import PartitionSpec as P

KP = 256
PANELS = 4
DOT = 1024
MESH = pl.DeviceIdType.MESH


def kernel(
    rows_n, cols_n, order, pieces, x_ref, out_ref, frob_ref, right, left, halves, weights, part_col, part_row,
    local_sem, z_recv, z_up, z_down, pair_send, pair_recv, hop_send, hop_recv, relay_send, relay_recv,
    col_send, col_recv, row_send, row_recv,
):
    row = lax.axis_index("row")
    col = lax.axis_index("col")
    chip = col // 2
    core = col % 2
    partner = chip * 2 + 1 - core
    row_block, col_block = out_ref.shape
    half = row_block // 2
    width = col_block // pieces

    barrier = pltpu.get_barrier_semaphore()
    for d in range(1, cols_n):
        pl.semaphore_signal(barrier, inc=1, device_id=(row, lax.rem(col + d, cols_n)), device_id_type=MESH)
    for d in range(1, rows_n):
        pl.semaphore_signal(barrier, inc=1, device_id=(lax.rem(row + d, rows_n), col), device_id_type=MESH)
    pl.semaphore_wait(barrier, rows_n + cols_n - 2)

    def columns(j):
        return pl.ds(pl.multiple_of(j * width, width), width)

    def z_copy(s, j, sems, target, own):
        view = right.at[s, :, columns(j)]
        source = x_ref.at[pl.ds(0, KP), columns(j)] if own else view
        return pltpu.make_async_remote_copy(
            src_ref=source, dst_ref=view, send_sem=sems.at[s, j], recv_sem=z_recv.at[s, j],
            device_id=(target, col), device_id_type=MESH,
        )

    above = lax.min(row + 1, rows_n - 1)
    below = lax.max(row - 1, 0)
    has_above = row < rows_n - 1
    has_below = row > 0

    def start_own(j, carry):
        @pl.when(has_above)
        def _():
            z_copy(row, j, z_up, above, True).start()

        @pl.when(has_below)
        def _():
            z_copy(row, j, z_down, below, True).start()

        return carry

    lax.fori_loop(0, pieces, start_own, 0)

    def pair_copy():
        return pltpu.make_async_remote_copy(
            src_ref=x_ref.at[:, pl.ds(0, KP)], dst_ref=left.at[chip], send_sem=pair_send, recv_sem=pair_recv,
            device_id=(row, partner), device_id_type=MESH,
        )

    def flip(q, d):
        hi, lo = q // 2, q % 2
        hi = hi if d < 2 else 1 - hi
        lo = lo if d % 2 == 0 else 1 - lo
        return hi * 2 + lo

    def hop_copy(d, h):
        rows = pl.ds(h * half, half)
        return pltpu.make_async_remote_copy(
            src_ref=x_ref.at[rows, pl.ds(0, KP)], dst_ref=left.at[chip, rows, :],
            send_sem=hop_send.at[d, h], recv_sem=hop_recv.at[chip],
            device_id=(row, flip(chip, d) * 2 + h), device_id_type=MESH,
        )

    @pl.when(core == 0)
    def _():
        for d in (1, 2, 3):
            for h in (0, 1):
                hop_copy(d, h).start()
        pair_copy().start()

    own_right = pltpu.make_async_copy(x_ref.at[pl.ds(0, KP), :], right.at[row], local_sem.at[0])
    own_left = pltpu.make_async_copy(x_ref.at[:, pl.ds(0, KP)], left.at[chip], local_sem.at[1])
    own_right.start()

    @pl.when(core == 0)
    def _():
        own_left.start()

    tile = 256
    tiles = row_block // tile

    def clear(i, carry):
        out_ref[pl.ds(pl.multiple_of(i * tile, tile), tile), :] = jnp.zeros((tile, col_block), jnp.float32)
        return carry

    lax.fori_loop(0, tiles, clear, 0)

    def split(s):
        def one(i, carry):
            rows = pl.ds(pl.multiple_of(i * tile, tile), tile)
            value = left[s, rows, :]
            head = value.astype(jnp.bfloat16)
            halves[s, rows, pl.ds(0, KP)] = head
            halves[s, rows, pl.ds(KP, KP)] = (value - head.astype(jnp.float32)).astype(jnp.bfloat16)
            return carry

        lax.fori_loop(0, tiles, one, 0)

    def multiply(first, count, j, add):
        cols = columns(j)
        for i in range(count):
            value = right[first + i, :, cols]
            head = value.astype(jnp.bfloat16)
            weights[pl.ds(3 * KP * i, KP), :] = head
            weights[pl.ds(3 * KP * i + KP, KP), :] = head
            weights[pl.ds(3 * KP * i + 2 * KP, KP), :] = (value - head.astype(jnp.float32)).astype(jnp.bfloat16)

        def one(i, carry):
            rows = pl.ds(pl.multiple_of(i * DOT, DOT), DOT)
            pieces_of = []
            for p in range(count):
                pieces_of += [halves[first + p, rows, :], halves[first + p, rows, pl.ds(0, KP)]]
            value = jnp.dot(
                jnp.concatenate(pieces_of, axis=1), weights[pl.ds(0, 3 * KP * count), :],
                preferred_element_type=jnp.float32,
            )
            out_ref[rows, cols] = value + out_ref[rows, cols] if add else value
            return carry

        lax.fori_loop(0, row_block // DOT, one, 0)

    def receive(k, j):
        @pl.when(row >= k)
        def _():
            s = lax.max(row - k, 0)
            z_copy(s, j, z_up, above, False).wait_recv()

            @pl.when(has_above)
            def _():
                z_copy(s, j, z_up, above, False).start()

        @pl.when(row + k < rows_n)
        def _():
            s = lax.min(row + k, rows_n - 1)
            z_copy(s, j, z_down, below, False).wait_recv()

            @pl.when(has_below)
            def _():
                z_copy(s, j, z_down, below, False).start()

    mine = pl.ds(pl.multiple_of(core * half, half), half)
    other = pl.ds(pl.multiple_of((1 - core) * half, half), half)

    def relay_copy(s, rows):
        return pltpu.make_async_remote_copy(
            src_ref=left.at[s, rows, :], dst_ref=left.at[s, rows, :], send_sem=relay_send.at[s],
            recv_sem=relay_recv.at[s], device_id=(row, partner), device_id_type=MESH,
        )

    def hop_arrival(s):
        view = left.at[s, mine, :]
        return pltpu.make_async_remote_copy(
            src_ref=view, dst_ref=view, send_sem=hop_send.at[0, 0], recv_sem=hop_recv.at[s],
            device_id=(row, partner), device_id_type=MESH,
        )

    def relay(distances):
        for d in distances:
            s = flip(chip, d)
            hop_arrival(s).wait_recv()
            relay_copy(s, mine).start()
        for d in distances:
            s = flip(chip, d)
            relay_copy(s, other).wait_recv()
            relay_copy(s, mine).wait_send()
            split(s)

    own_right.wait()

    @pl.when(core == 0)
    def _():
        own_left.wait()

    @pl.when(core == 1)
    def _():
        pair_copy().wait_recv()

    split(chip)

    def step(k):
        def one(j, carry):
            receive(k, j)
            return carry

        lax.fori_loop(0, pieces, one, 0)

    step(1)
    relay((1, 2))
    low_end = row < rows_n // 2
    first = jnp.where(low_end, 0, 1)
    farthest = jnp.where(low_end, rows_n - 1, 0)
    diagonal = flip(chip, 3)

    def near(j, carry):
        receive(2, j)
        for i in range(PANELS - 1):
            @pl.when(first + i != diagonal)
            def _():
                multiply(first + i, 1, j, True)

        return carry

    lax.fori_loop(0, pieces, near, 0)
    relay((3,))

    @pl.when(diagonal != farthest)
    def _():
        def one(j, carry):
            multiply(diagonal, 1, j, True)
            return carry

        lax.fori_loop(0, pieces, one, 0)


    def last(j, total):
        receive(rows_n - 1, j)
        multiply(farthest, 1, j, True)
        cols = columns(j)

        def one(i, acc):
            value = out_ref[pl.ds(pl.multiple_of(i * tile, tile), tile), cols]
            value = value * value
            return acc + jnp.sum(value.reshape(tile // 8, 8, width), axis=0)

        return lax.fori_loop(0, tiles, one, total)

    total = lax.fori_loop(0, pieces, last, jnp.zeros((8, width), jnp.float32))
    part_col[col] = sum(total[:, i * 128 : (i + 1) * 128] for i in range(width // 128))

    def drain(j, carry):
        @pl.when(has_above)
        def _():
            z_copy(row, j, z_up, above, True).wait_send()

        @pl.when(has_below)
        def _():
            z_copy(row, j, z_down, below, True).wait_send()

        for k in range(1, rows_n):
            @pl.when(jnp.logical_and(row >= k, has_above))
            def _():
                z_copy(lax.max(row - k, 0), j, z_up, above, False).wait_send()

            @pl.when(jnp.logical_and(row + k < rows_n, has_below))
            def _():
                z_copy(lax.min(row + k, rows_n - 1), j, z_down, below, False).wait_send()

        return carry

    lax.fori_loop(0, pieces, drain, 0)

    @pl.when(core == 0)
    def _():
        for d in (1, 2, 3):
            for h in (0, 1):
                hop_copy(d, h).wait_send()
        pair_copy().wait_send()

    def spread(part, place, count, send, recv, device):
        def copy(d, slot):
            return pltpu.make_async_remote_copy(
                src_ref=part.at[slot], dst_ref=part.at[slot], send_sem=send.at[d], recv_sem=recv.at[slot],
                device_id=device(lax.rem(place + d, count)), device_id_type=MESH,
            )

        for d in range(1, count):
            copy(d, place).start()
        for d in range(1, count):
            copy(d, lax.rem(place + d, count)).wait_recv()
        for d in range(1, count):
            copy(d, place).wait_send()

    spread(part_col, col, cols_n, col_send, col_recv, lambda c: (row, c))
    part_row[row] = jnp.sum(part_col[...], axis=0)
    spread(part_row, row, rows_n, row_send, row_recv, lambda r: (r, col))
    full = jnp.sum(jnp.sum(part_row[...], axis=0), keepdims=True)
    frob_ref[...] = jnp.sqrt(full) / order


def fused(rows_n, cols_n, matrix):
    row_block, col_block = matrix.shape
    order = row_block * rows_n
    pieces = max(1, col_block // 256)
    dma = pltpu.SemaphoreType.DMA
    vmem = pl.BlockSpec(memory_space=pltpu.VMEM)
    squared, frob = pl.pallas_call(
        functools.partial(kernel, rows_n, cols_n, order, pieces),
        out_shape=(
            pltpu.VMEM((row_block, col_block), jnp.float32),
            jax.ShapeDtypeStruct((1, 1), jnp.float32),
        ),
        in_specs=[pl.BlockSpec(memory_space=pltpu.HBM)],
        out_specs=(vmem, vmem),
        scratch_shapes=[
            pltpu.VMEM((PANELS, KP, col_block), jnp.float32),
            pltpu.VMEM((PANELS, row_block, KP), jnp.float32),
            pltpu.VMEM((PANELS, row_block, 2 * KP), jnp.bfloat16),
            pltpu.VMEM((3 * KP, col_block // pieces), jnp.bfloat16),
            pltpu.VMEM((cols_n, 8, 128), jnp.float32),
            pltpu.VMEM((rows_n, 8, 128), jnp.float32),
            dma((2,)), dma((PANELS, pieces)), dma((PANELS, pieces)), dma((PANELS, pieces)),
            dma(()), dma(()), dma((PANELS, 2)), dma((PANELS,)), dma((PANELS,)), dma((PANELS,)),
            dma((cols_n,)), dma((cols_n,)), dma((rows_n,)), dma((rows_n,)),
        ],
        compiler_params=pltpu.CompilerParams(
            collective_id=0, has_side_effects=True, vmem_limit_bytes=52 * 1024 * 1024
        ),
    )(matrix)
    return squared, frob.reshape(())


def broadcast(value, axis, source):
    kept = jnp.where(lax.axis_index(axis) == source, value, 0).astype(value.dtype)
    return lax.psum(kept, axis)


def offsets(matrix, step):
    row_block = matrix.shape[0]
    col_block = matrix.shape[1]
    total = row_block * lax.axis_size("row")
    start = step * (total // PANELS)
    return (start // col_block, start % col_block, start // row_block, start % row_block)


def fetch_rows(matrix, step):
    col_owner, local_col, row_owner, local_row = offsets(matrix, step)
    return broadcast(matrix[local_row : local_row + KP, :], "row", row_owner)


def product(left, right):
    return jnp.dot(left, right, preferred_element_type=jnp.float32, precision=lax.Precision.HIGHEST)


def general(matrix):
    column_index = lax.axis_index("col")
    slots = []
    for step in range(PANELS):
        col_owner, local_col, row_owner, local_row = offsets(matrix, step)
        panel = matrix[:, local_col : local_col + KP]
        slots.append(jnp.where(column_index == col_owner, panel, jnp.zeros_like(panel)))
    stacked = lax.psum(jnp.concatenate(slots, axis=1), "col")
    rights = jnp.concatenate([fetch_rows(matrix, step) for step in range(PANELS)], axis=0)
    squared = product(stacked, rights)
    total = lax.psum(jnp.sum(squared * squared), ("row", "col"))
    order_size = matrix.shape[0] * lax.axis_size("row")
    frob = jnp.sqrt(total) / order_size
    return (squared, frob)


def solution(mesh):
    rows_n, cols_n = mesh.shape["row"], mesh.shape["col"]
    if rows_n == PANELS and cols_n == 2 * PANELS:
        body = functools.partial(fused, rows_n, cols_n)
    else:
        body = general
    return jax.shard_map(
        body, mesh=mesh, in_specs=(P("row", "col"),), out_specs=(P("row", "col"), P()), check_vma=False
    )
```
